32 devices in a mesh: groups: 2 (over x), az: 16 (over z, y, core).
Axes of the slice: x: 2, y: 2, z: 4, core: 2. Of those that a mesh axis runs over, the one named last changes fastest.
Arguments:
- raw_first: bfloat16 [4, 8192, 8192], P('groups', 'az'), parts along dimension 0, may hold values from -6 to 6
- raw_second: bfloat16 [4, 8192, 8192], P('groups', 'az'), parts along dimension 0, may hold values from -6 to 6
- offsets: int32 [4], P('groups'), parts along dimension 0, may hold values from -16 to 16
- chirp_lengths: int32 [4], P('groups'), parts along dimension 0, may hold values from 256 to 2048
Outputs:
- interferogram: float32 [4, 1024, 8192], P('groups', 'az'), parts along dimension 0
- coherence: float32 [2048, 8192], P(('groups', 'az')), parts along dimension 0
The draws below stay inside these ranges and needn't reach their ends.
There are 2 independent parts, one for each index of `groups`. The reference program is written for one: setup_inputs(seed, part) draws one part's arguments, and reference() takes and returns one part's arrays. A program takes and returns all parts, laid end to end along the dimension named above; each array names one. Nothing has to cross between parts.
Inputs may be any that keep to these rules, and one draw needn't show every extreme that they name: offsets[0] shifts azimuth lines, offsets[1] range bins. chirp_lengths[0] is the range chirp, chirp_lengths[1] the azimuth chirp.
All inputs are finite; a program needn't handle non-finite values.
Results may differ from the reference program's by a relative error of at most 0.0003.
Values sent between devices are 32-bit elements; how exact they have to be, the bound alone decides.
No kernel may reach another device: no remote copies, remote signals or barrier semaphores. Data moves between devices by JAX's collectives and lax.ppermute only.
A program may use at most 256 MiB of HBM per device.

```python
import jax
import jax.numpy as jnp
from jax import lax

NAZ = 8192
NRG = 8192
WINDOW = 1024
MAXSHIFT = 16


def block_levels(key, shape, cuts, least, top_value):
    gain, own = 1.0, jax.random.fold_in(key, 6)
    for position, parts in cuts:
        heights = jnp.exp(jax.random.uniform(jax.random.fold_in(own, position), (parts,), jnp.float32, least / len(cuts), top_value / len(cuts)))
        gain = gain * jnp.repeat(heights, shape[position] // parts).reshape([-1 if axis == position else 1 for axis in range(len(shape))])
    return gain


def bell_draw(rng, dims, spread, limit, cuts=(), kind=jnp.bfloat16):
    loudness = block_levels(rng, dims, cuts, -0.22, 0.18) if cuts else 1.0
    drawn = jax.random.normal(rng, dims, jnp.float32) * spread * loudness
    return jnp.minimum(jnp.maximum(drawn, -limit), limit).astype(kind)


def setup_inputs(seed: int = 0, part: int = 0) -> dict:
    arg_keys = jax.random.split(jax.random.key(seed), 5)
    part_keys = jax.random.split(jax.random.fold_in(arg_keys[4], part), 5)
    raw_first = bell_draw(part_keys[0], (2, NAZ, NRG), 1.0, 6.0, ((1, 16),))
    raw_second = bell_draw(part_keys[1], (2, NAZ, NRG), 1.0, 6.0, ((1, 16),))
    offsets = jax.random.randint(part_keys[2], (2,), 0 - MAXSHIFT, MAXSHIFT + 1).astype(jnp.int32)
    chirp_lengths = jax.random.randint(part_keys[3], (2,), min(NRG, NAZ) // 32, min(NRG, NAZ) // 4 + 1).astype(jnp.int32)
    return dict(raw_first=raw_first, raw_second=raw_second, offsets=offsets, chirp_lengths=chirp_lengths)


def chirp(length, samples_all):
    sample = jnp.arange(samples_all, dtype=jnp.int32)
    offset = 2 * sample - length
    period = 8 * length
    numerator = jnp.mod(offset * offset, period)
    angles = jnp.pi * numerator.astype(jnp.float32) / (4 * length).astype(jnp.float32)
    amplitude = jnp.where(sample < length, 1.0 / jnp.sqrt(length.astype(jnp.float32)), 0.0).astype(jnp.float32)
    return (amplitude * jnp.cos(angles), amplitude * jnp.sin(angles))

def boxed(values):
    rows_count, cols_count = values.shape
    padded = jnp.pad(values, ((3, 4), (3, 4)))
    across = padded[0:rows_count]
    for offset_row in range(1, 8):
        across = across + padded[offset_row:offset_row + rows_count]
    result = across[:, 0:cols_count]
    for offset_col in range(1, 8):
        result = result + across[:, offset_col:offset_col + cols_count]
    return result

def focus(raw, range_filter, azimuth_filter):
    signal = lax.complex(raw[0].astype(jnp.float32), raw[1].astype(jnp.float32))
    signal = jnp.fft.ifft(jnp.fft.fft(signal, axis=1) * range_filter[None, :], axis=1)
    return jnp.fft.ifft(jnp.fft.fft(signal, axis=0) * azimuth_filter[:, None], axis=0)

def reference(raw_first, raw_second, offsets, chirp_lengths):
    range_real, range_imag = chirp(chirp_lengths[0], NRG)
    range_filter = jnp.conj(jnp.fft.fft(lax.complex(range_real, range_imag)))
    azimuth_real, azimuth_imag = chirp(chirp_lengths[1], NAZ)
    azimuth_filter = jnp.conj(jnp.fft.fft(lax.complex(azimuth_real, azimuth_imag)))
    first = focus(raw_first, range_filter, azimuth_filter)[:, 0:WINDOW]
    second = focus(raw_second, range_filter, azimuth_filter)
    padded = jnp.pad(second, MAXSHIFT)
    second = lax.dynamic_slice(padded, ((MAXSHIFT - offsets[0]).astype(jnp.int32), (MAXSHIFT - offsets[1]).astype(jnp.int32)), (NAZ, WINDOW))
    cross = first * jnp.conj(second)
    sums_real = boxed(jnp.real(cross))
    sums_imag = boxed(jnp.imag(cross))
    power_first = boxed(jnp.real(first) * jnp.real(first) + jnp.imag(first) * jnp.imag(first))
    power_second = boxed(jnp.real(second) * jnp.real(second) + jnp.imag(second) * jnp.imag(second))
    coherence = jnp.sqrt(sums_real * sums_real + sums_imag * sums_imag) / jnp.sqrt(power_first * power_second + 1.0)
    interferogram = jnp.stack([sums_real.T, sums_imag.T]) / 64.0
    return (interferogram, coherence.T)
```

```python
import functools
import math

import jax
import jax.numpy as jnp
from jax import lax
from jax.experimental import pallas as pl
from jax.experimental.pallas import tpu as pltpu
from jax.sharding import PartitionSpec as P

WINDOW = 1024
MAXSHIFT = 16
SPAN = 256
HALF = 128
LIMIT = 60 * 1024 * 1024

F32, BF16 = jnp.float32, jnp.bfloat16


def chirps(lengths, samples):
    sample = lax.broadcasted_iota(jnp.int32, (2, samples), 1)
    length = lengths[:, None]
    offset = 2 * sample - length
    numerator = jnp.mod(offset * offset, 8 * length)
    angles = jnp.pi * numerator.astype(F32) / (4 * length).astype(F32)
    amplitude = jnp.where(sample < length, 1.0 / jnp.sqrt(length.astype(F32)), 0.0)
    return amplitude * jnp.cos(angles), amplitude * jnp.sin(angles)


def table_kernel(plan, offs_ref, real_ref, imag_ref, *refs):
    outs, scratch = refs[:-1], refs[-1]
    for (row, which, lead, depth, starts), out in zip(plan, outs):
        cols = 8 * len(starts)
        base = lead - offs_ref[which] if lead else 0
        for part, ref in enumerate((real_ref, imag_ref)):
            line = jnp.broadcast_to(ref[row : row + 1, 0:depth], (8, depth))
            line = pltpu.roll(line, 0, 1, stride=1, stride_axis=0)
            uniform = all(start == 8 * k for k, start in enumerate(starts))
            if uniform and len(starts) > 8:

                @pl.loop(0, len(starts))
                def _(k):
                    moved = pltpu.roll(line, base + 8 * k, 1)
                    scratch[pl.ds(pl.multiple_of(part * cols + 8 * k, 8), 8), 0:depth] = moved

            else:
                for k, start in enumerate(starts):
                    moved = pltpu.roll(line, base + start, 1)
                    scratch[part * cols + 8 * k : part * cols + 8 * k + 8, 0:depth] = moved

        @pl.loop(0, depth // HALF)
        def _(k):
            at = pl.ds(pl.multiple_of(k * HALF, HALF), HALF)
            turned = scratch[0 : 2 * cols, at].T
            high = turned.astype(BF16)
            out[at, 0 : 2 * cols] = high
            out[at, 2 * cols : 4 * cols] = (turned - high.astype(F32)).astype(BF16)


def make_tables(plan, offsets, real, imag):
    rows = max(2 * 8 * len(item[4]) for item in plan)
    depth = max(item[3] for item in plan)
    size = sum(item[3] * 32 * len(item[4]) for item in plan)
    vmem = pl.BlockSpec(memory_space=pltpu.VMEM)
    return pl.pallas_call(
        functools.partial(table_kernel, plan),
        out_shape=[jax.ShapeDtypeStruct((item[3], 32 * len(item[4])), BF16) for item in plan],
        in_specs=[pl.BlockSpec(memory_space=pltpu.SMEM), vmem, vmem],
        out_specs=[vmem] * len(plan),
        scratch_shapes=[pltpu.VMEM((rows, depth), F32)],
        compiler_params=pltpu.CompilerParams(vmem_limit_bytes=LIMIT),
        cost_estimate=pl.CostEstimate(flops=size * 200, bytes_accessed=2 * size, transcendentals=0),
        name="tables",
    )(offsets, real, imag)


def range_kernel(plan, sizes, offs_ref, first_ref, second_ref, *refs):
    tables, out = refs[0:2], refs[2]
    windows, share, bins = sizes
    lines = out.shape[3]
    cols = share * len(bins) * 8
    for side, (source, table) in enumerate(zip((first_ref, second_ref), tables)):
        lead, depth = plan[side]

        def piece(start, stop):
            return source[:, :, start:stop].reshape(2 * lines, stop - start)

        for window in range(windows):
            start = SPAN * window - lead
            if start < 0:
                left = jnp.concatenate(
                    [jnp.zeros((2 * lines, -start), BF16), piece(0, start + depth)], axis=1
                )
            else:
                left = piece(start, start + depth)
            both = jnp.dot(left, table[...], preferred_element_type=F32)
            turned = (both[:, 0 : 2 * cols] + both[:, 2 * cols :]).T
            real = turned[0:cols, 0:lines] + turned[cols:, lines:]
            imag = turned[0:cols, lines:] - turned[cols:, 0:lines]
            real = real.reshape(share, len(bins) * 8, lines)
            imag = imag.reshape(share, len(bins) * 8, lines)
            if side and start < 0:
                shape = (share, 8, lines)
                own = lax.broadcasted_iota(jnp.int32, shape, 0) * (SPAN // share)
                own = own + lax.broadcasted_iota(jnp.int32, shape, 1)
                index = jnp.concatenate([own + item for item in bins], axis=1)
                inside = index >= offs_ref[1]
                real = jnp.where(inside, real, 0.0)
                imag = jnp.where(inside, imag, 0.0)
            out[window * share : (window + 1) * share, 2 * side] = real
            out[window * share : (window + 1) * share, 2 * side + 1] = imag


def range_focus(plan, sizes, count, offsets, first, second, tables):
    windows, share, bins = sizes
    lines_all = first.shape[1]
    lines = min(lines_all, SPAN)
    reach = max(SPAN * (windows - 1) - lead + depth for lead, depth in plan)
    block = pl.BlockSpec((2, lines, reach), lambda i: (0, i, 0))
    whole = pl.BlockSpec(memory_space=pltpu.VMEM)
    flops = sum(2 * 2 * lines_all * windows * depth * tables[0].shape[1] for _, depth in plan)
    return pl.pallas_call(
        functools.partial(range_kernel, plan, sizes),
        grid=(lines_all // lines,),
        out_shape=jax.ShapeDtypeStruct((count, 4, 8 * len(bins), lines_all), F32),
        in_specs=[pl.BlockSpec(memory_space=pltpu.SMEM), block, block, whole, whole],
        out_specs=pl.BlockSpec((count, 4, 8 * len(bins), lines), lambda i: (0, 0, 0, i)),
        compiler_params=pltpu.CompilerParams(vmem_limit_bytes=LIMIT),
        cost_estimate=pl.CostEstimate(flops=flops, bytes_accessed=16 << 20, transcendentals=0),
        name="ranges",
    )(offsets, first, second, *tables)


def azimuth_kernel(depth, group, offs_ref, got_ref, table, out, high, low, image):
    sources, _, bins, width = got_ref.shape
    spans = width // SPAN
    windows = sources * spans
    lines_all = windows * SPAN
    extra = high.shape[1] - windows
    cols = table.shape[1] // 2

    @pl.loop(0, sources)
    def _(source):
        for side in range(2):
            for part in range(spans):
                block = got_ref[
                    source, 2 * side : 2 * side + 2, :, part * SPAN : (part + 1) * SPAN
                ].reshape(2 * bins, SPAN)
                upper = block.astype(BF16)
                high[side, source * spans + part] = upper
                low[side, source * spans + part] = (block - upper.astype(F32)).astype(BF16)

    for side in range(2):
        for slot in range(extra):
            high[side, windows + slot] = high[side, slot % windows]
            low[side, windows + slot] = low[side, slot % windows]

    pads = jnp.zeros((4, bins, HALF), F32)
    image[:, :, 0:HALF] = pads
    image[:, :, HALF + lines_all :] = pads

    @pl.loop(0, 2 * (windows // group))
    def _(turn):
        side = turn // (windows // group)
        base = (turn % (windows // group)) * group

        def gathered(ref):
            pieces = []
            for unit in range(depth // SPAN):
                taken = ref[side, pl.ds(base + unit, group)]
                pieces.append(taken.reshape(group * 2 * bins, SPAN))
            return jnp.concatenate(pieces, axis=1)

        upper, lower = gathered(high), gathered(low)
        both = jnp.dot(upper, table[:, 0:cols], preferred_element_type=F32)
        both += jnp.dot(lower, table[:, 0:cols], preferred_element_type=F32)
        both += jnp.dot(upper, table[:, cols:], preferred_element_type=F32)
        both = both.reshape(group, 2, bins, cols)
        real = both[:, 0, :, 0:SPAN] + both[:, 1, :, SPAN:]
        imag = both[:, 1, :, 0:SPAN] - both[:, 0, :, SPAN:]
        for k in range(group):
            at = pl.ds(pl.multiple_of((base + k) * SPAN + HALF, HALF), SPAN)
            image[2 * side, :, at] = real[k]
            image[2 * side + 1, :, at] = imag[k]

    block = math.gcd(lines_all, 1024)
    length = block + 2 * HALF
    shift = jnp.where(offs_ref[0] < 0, offs_ref[0] + length, offs_ref[0])

    @pl.loop(0, lines_all // block)
    def _(step):
        start = pl.multiple_of(step * block, HALF)
        at = pl.ds(start, length)
        for row in range(0, bins, 8):
            rows = slice(row, row + 8)
            a, b = image[0, rows, at], image[1, rows, at]
            c = pltpu.roll(image[2, rows, at], shift, 1)
            d = pltpu.roll(image[3, rows, at], shift, 1)
            fields = (a * c + b * d, b * c - a * d, a * a + b * b, c * c + d * d)
            for k, value in enumerate(fields):
                line = lax.broadcasted_iota(jnp.int32, (8, length), 1) + (start - HALF)
                if k == 3:
                    value = jnp.where((line >= 0) & (line < lines_all), value, 0.0)
                for hop in (1, 2, 4):
                    value = value + pltpu.roll(value, length - hop, 1)
                out[k, rows, pl.ds(start, block)] = pltpu.roll(value, 3, 1)[:, HALF : HALF + block]


def azimuth_focus(depth, offsets, got, table):
    sources, _, bins, width = got.shape
    windows = sources * width // SPAN
    lines_all = windows * SPAN
    group = math.gcd(windows, max(1, 512 // (2 * bins)))
    vmem = pl.BlockSpec(memory_space=pltpu.VMEM)
    store = pltpu.VMEM((2, windows + depth // SPAN - 1, 2 * bins, SPAN), BF16)
    flops = 2 * 2 * 3 * windows * 2 * bins * depth * 2 * SPAN
    return pl.pallas_call(
        functools.partial(azimuth_kernel, depth, group),
        out_shape=jax.ShapeDtypeStruct((4, bins, lines_all), F32),
        in_specs=[pl.BlockSpec(memory_space=pltpu.SMEM)] + [vmem] * 2,
        out_specs=vmem,
        scratch_shapes=[store, store, pltpu.VMEM((4, bins, lines_all + 2 * HALF), F32)],
        compiler_params=pltpu.CompilerParams(vmem_limit_bytes=LIMIT),
        cost_estimate=pl.CostEstimate(flops=flops, bytes_accessed=8 << 20, transcendentals=0),
        name="azimuths",
    )(offsets, got, table)


def finish_kernel(layout, below_ref, above_ref, *refs):
    parts = refs[: len(layout)]
    picture, coherence, held = refs[len(layout) :]
    bins = coherence.shape[0]
    held[:, 0:3] = below_ref[:, 1:4]
    held[:, 3 + bins : 7 + bins] = above_ref[...]
    for part, starts in zip(parts, layout):
        for k, start in enumerate(starts):
            held[:, 3 + start : 11 + start] = part[:, 8 * k : 8 * k + 8]
    sums = []
    for field in range(4):
        total = held[field]
        for hop in (1, 2, 4):
            total = total + pltpu.roll(total, bins + 8 - hop, 0)
        sums.append(total[0:bins])
    picture[0] = sums[0] * (1.0 / 64.0)
    picture[1] = sums[1] * (1.0 / 64.0)
    coherence[...] = jnp.sqrt(sums[0] * sums[0] + sums[1] * sums[1]) / jnp.sqrt(sums[2] * sums[3] + 1.0)


def finish(layout, below, above, parts):
    lines_all = below.shape[2]
    bins = sum(part.shape[1] for part in parts)
    block = math.gcd(lines_all, 512)
    spec = lambda rows: pl.BlockSpec((4, rows, block), lambda i: (0, 0, i))
    return pl.pallas_call(
        functools.partial(finish_kernel, layout),
        grid=(lines_all // block,),
        out_shape=[
            jax.ShapeDtypeStruct((2, bins, lines_all), F32),
            jax.ShapeDtypeStruct((bins, lines_all), F32),
        ],
        in_specs=[spec(4), spec(4)] + [spec(part.shape[1]) for part in parts],
        out_specs=[
            pl.BlockSpec((2, bins, block), lambda i: (0, 0, i)),
            pl.BlockSpec((bins, block), lambda i: (0, i)),
        ],
        scratch_shapes=[pltpu.VMEM((4, bins + 8, block), F32)],
        compiler_params=pltpu.CompilerParams(vmem_limit_bytes=LIMIT),
        cost_estimate=pl.CostEstimate(flops=100 * bins * lines_all, bytes_accessed=16 << 20, transcendentals=0),
        name="finish",
    )(below, above, *parts)


def chunks_of(bins):
    if bins < 64:
        return [tuple(range(0, bins, 8))]
    inner = list(range(8, bins - 8, 8))
    return [(0, bins - 8), tuple(inner[:-2]), tuple(inner[-2:])]


def on_device(raw_first, raw_second, offsets, chirp_lengths):
    count = lax.axis_size("az")
    lines, range_count = raw_first.shape[1:]
    lines_all = lines * count
    reach = min(range_count, lines_all) // 4
    bins = WINDOW // count
    share = SPAN // bins
    plan = ((0, reach + SPAN), (HALF, reach + 2 * SPAN))
    real, imag = chirps(chirp_lengths, reach + 2 * SPAN)
    layout = chunks_of(bins)

    def columns(starts):
        return tuple(bins * k + start for k in range(share) for start in starts)

    def tables(row, starts, offset):
        return tuple((row, offset, lead, depth, starts) for lead, depth in plan)

    def turned(got):
        width = got.shape[3]
        if width % SPAN:
            fold = SPAN // width
            got = got.reshape(count // fold, fold, 4, got.shape[2], width)
            got = got.transpose(0, 2, 3, 1, 4).reshape(count // fold, 4, got.shape[3], SPAN)
        return got

    sizes = [(WINDOW // SPAN, share, starts) for starts in layout]
    along = tuple(8 * k for k in range(SPAN // 8))
    table_sets = [tables(0, columns(starts), 1) for starts in layout]
    table_sets[min(1, len(layout) - 1)] += tables(1, along, 0)[0:1]
    parts, given, azimuth_table = [], (offsets, real, imag), None
    exchanged = []
    for index, size in enumerate(sizes):
        made = make_tables(table_sets[index], *given)
        azimuth_table = made[2] if len(made) > 2 else azimuth_table
        sent = range_focus(plan, size, count, given[0], raw_first, raw_second, made[0:2])
        if exchanged:
            given, sent, exchanged[-1] = lax.optimization_barrier((given, sent, exchanged[-1]))
        else:
            given, sent = lax.optimization_barrier((given, sent))
        exchanged.append(lax.all_to_all(sent, "az", split_axis=0, concat_axis=0, tiled=True))
    for got in exchanged:
        parts.append(azimuth_focus(plan[0][1], offsets, turned(got), azimuth_table))
    up = [(i, i + 1) for i in range(count - 1)]
    down = [(j, i) for i, j in up]
    edge = parts[0]
    below = lax.ppermute(edge[:, edge.shape[1] - 4 :], "az", up)
    above = lax.ppermute(edge[:, 0:4], "az", down)
    return tuple(finish(layout, below, above, parts))


def solution(mesh):
    in_specs = (P("groups", "az", None), P("groups", "az", None), P("groups"), P("groups"))
    out_specs = (P("groups", "az", None), P(("groups", "az"), None))
    return jax.shard_map(
        on_device, mesh=mesh, in_specs=in_specs, out_specs=out_specs, check_vma=False
    )
```

```python
import functools
import math

import jax
import jax.numpy as jnp
from jax import lax
from jax.experimental import pallas as pl
from jax.experimental.pallas import tpu as pltpu
from jax.sharding import PartitionSpec as P

WINDOW = 1024
MAXSHIFT = 16
SPAN = 256
HALF = 128
LIMIT = 60 * 1024 * 1024
ROOMY = 22 * 1024 * 1024

F32, BF16 = jnp.float32, jnp.bfloat16


def chirp_lines(length, depth):
    shape = (8, depth)
    sample = lax.broadcasted_iota(jnp.int32, shape, 1) - lax.broadcasted_iota(jnp.int32, shape, 0)
    held = (sample >= 0) & (sample < length)
    offset = jnp.where(held, 2 * sample - length, 0)
    square = offset * offset
    period = jnp.full(shape, 8 * length, jnp.int32)
    whole = (square.astype(F32) / period.astype(F32)).astype(jnp.int32)
    numerator = square - whole * period
    numerator = jnp.where(numerator < 0, numerator + period, numerator)
    numerator = jnp.where(numerator >= period, numerator - period, numerator)
    size = period.astype(F32) * 0.125
    angles = jnp.pi * numerator.astype(F32) / (4.0 * size)
    amplitude = jnp.where(held, 1.0 / jnp.sqrt(size), 0.0)
    return amplitude * jnp.cos(angles), amplitude * jnp.sin(angles)


def table_kernel(plan, offs_ref, lengths_ref, *refs):
    outs, scratch = refs[:-1], refs[-1]
    for (row, shifted, lead, depth, starts), out in zip(plan, outs):
        cols = 8 * len(starts)
        base = lead - offs_ref[1] if shifted else lead
        uniform = len(starts) > 8 and all(start == 8 * k for k, start in enumerate(starts))
        for part, line in enumerate(chirp_lines(lengths_ref[row], depth)):
            if uniform:
                held = line

                @pl.loop(0, len(starts))
                def _(k):
                    moved = pltpu.roll(held, base + 8 * k, 1)
                    scratch[pl.ds(pl.multiple_of(part * cols + 8 * k, 8), 8), 0:depth] = moved

            else:
                for k, start in enumerate(starts):
                    moved = pltpu.roll(line, base + start, 1)
                    scratch[part * cols + 8 * k : part * cols + 8 * k + 8, 0:depth] = moved

        @pl.loop(0, depth // HALF)
        def _(k):
            at = pl.ds(pl.multiple_of(k * HALF, HALF), HALF)
            turned = scratch[0 : 2 * cols, at].T
            if row:
                real, imag = turned[:, 0:cols], turned[:, cols:]
                turned = jnp.concatenate([real, real + imag, real - imag], axis=1)
            width = turned.shape[1]
            high = turned.astype(BF16)
            out[at, 0:width] = high
            out[at, width : 2 * width] = (turned - high.astype(F32)).astype(BF16)


def make_tables(plan, offsets, lengths):
    rows = max(2 * 8 * len(item[4]) for item in plan)
    depth = max(item[3] for item in plan)
    widths = [8 * len(item[4]) * (6 if item[0] else 4) for item in plan]
    size = sum(item[3] * width for item, width in zip(plan, widths))
    smem = pl.BlockSpec(memory_space=pltpu.SMEM)
    vmem = pl.BlockSpec(memory_space=pltpu.VMEM)
    return pl.pallas_call(
        functools.partial(table_kernel, plan),
        out_shape=[jax.ShapeDtypeStruct((item[3], width), BF16) for item, width in zip(plan, widths)],
        in_specs=[smem, smem],
        out_specs=[vmem] * len(plan),
        scratch_shapes=[pltpu.VMEM((rows, depth), F32)],
        compiler_params=pltpu.CompilerParams(vmem_limit_bytes=ROOMY if plan[0][0] else LIMIT),
        cost_estimate=pl.CostEstimate(flops=size * 400, bytes_accessed=2 * size, transcendentals=0),
        name="tables",
    )(offsets, lengths)


def range_kernel(plan, windows, share, groups, routes, looped, offs_ref, first_ref, second_ref, *refs):
    tables, outs = refs[0:2], refs[2:]
    lines = first_ref.shape[1]
    for side, (source, table) in enumerate(zip((first_ref, second_ref), tables)):
        lead, depth = plan[side]

        def run(window, source=source, table=table, side=side, lead=lead, depth=depth):
            still = isinstance(window, int)
            start = SPAN * window - lead
            if still and start < 0:
                empty = jnp.zeros((2 * lines, -start), BF16)
                inner = source[:, :, 0 : start + depth].reshape(2 * lines, start + depth)
                left = jnp.concatenate([empty, inner], axis=1)
            else:
                at = pl.ds(start if still else pl.multiple_of(start, HALF), depth)
                left = source[:, :, at].reshape(2 * lines, depth)
            for skip, eights in groups:
                cols = share * len(eights) * 8
                both = jnp.dot(left, table[skip : skip + depth], preferred_element_type=F32)
                turned = (both[:, 0 : 2 * cols] + both[:, 2 * cols :]).T
                real = turned[0:cols, 0:lines] + turned[cols:, lines:]
                imag = turned[0:cols, lines:] - turned[cols:, 0:lines]
                real = real.reshape(share, len(eights), 8, lines)
                imag = imag.reshape(share, len(eights), 8, lines)
                for k, eight in enumerate(eights):
                    pair = real[:, k], imag[:, k]
                    if side and still and window * SPAN + eight < MAXSHIFT:
                        shape = (share, 8, lines)
                        index = lax.broadcasted_iota(jnp.int32, shape, 0) * (SPAN // share)
                        index = index + lax.broadcasted_iota(jnp.int32, shape, 1)
                        inside = index + (window * SPAN + eight) >= offs_ref[1]
                        pair = [jnp.where(inside, value, 0.0) for value in pair]
                    chunk, slot = routes[eight]
                    for part, value in enumerate(pair):
                        place = pl.ds(window * share, share)
                        outs[chunk][place, 2 * side + part, 8 * slot : 8 * slot + 8] = value

        if looped:
            for window in range(side):
                run(window)
            pl.loop(side, windows)(run)
        else:
            for window in range(windows):
                run(window)


def range_focus(plan, share, groups, routes, looped, count, offsets, first, second, tables):
    windows = WINDOW // SPAN
    lines_all = first.shape[1]
    lines = min(lines_all, SPAN)
    reach = max(SPAN * (windows - 1) - lead + depth for lead, depth in plan)
    block = pl.BlockSpec((2, lines, reach), lambda i: (0, i, 0))
    whole = pl.BlockSpec(memory_space=pltpu.VMEM)
    sizes = [0] * (1 + max(chunk for chunk, _ in routes.values()))
    for chunk, _ in routes.values():
        sizes[chunk] += 8
    bins = sum(sizes)
    flops = sum(2 * 2 * lines_all * windows * depth * share * bins * 4 for _, depth in plan)
    return pl.pallas_call(
        functools.partial(range_kernel, plan, windows, share, groups, routes, looped),
        grid=(lines_all // lines,),
        out_shape=[jax.ShapeDtypeStruct((count, 4, size, lines_all), F32) for size in sizes],
        in_specs=[pl.BlockSpec(memory_space=pltpu.SMEM), block, block, whole, whole],
        out_specs=[pl.BlockSpec((count, 4, size, lines), lambda i: (0, 0, 0, i)) for size in sizes],
        compiler_params=pltpu.CompilerParams(vmem_limit_bytes=LIMIT),
        cost_estimate=pl.CostEstimate(flops=flops, bytes_accessed=16 << 20, transcendentals=0),
        name="ranges",
    )(offsets, first, second, *tables)


def azimuth_kernel(depth, group, offs_ref, got_ref, table, out, high, low, image):
    sources, _, bins, width = got_ref.shape
    spans = width // SPAN
    windows = sources * spans
    lines_all = windows * SPAN
    extra = high.shape[1] - windows
    rows = 2 * bins

    @pl.loop(0, sources)
    def _(source):
        for part in range(spans):
            at = slice(part * SPAN, (part + 1) * SPAN)
            real = jnp.concatenate([got_ref[source, 0, :, at], got_ref[source, 2, :, at]], axis=0)
            imag = jnp.concatenate([got_ref[source, 1, :, at], got_ref[source, 3, :, at]], axis=0)
            for kind, value in enumerate((real + imag, real, imag)):
                upper = value.astype(BF16)
                high[kind, source * spans + part] = upper
                low[kind, source * spans + part] = (value - upper.astype(F32)).astype(BF16)

    for kind in range(3):
        for slot in range(extra):
            high[kind, windows + slot] = high[kind, slot % windows]
            low[kind, windows + slot] = low[kind, slot % windows]

    pads = jnp.zeros((4, bins, HALF), F32)
    image[:, :, 0:HALF] = pads
    image[:, :, HALF + lines_all :] = pads

    @pl.loop(0, windows // group)
    def _(turn):
        base = turn * group

        def gathered(ref, kind):
            pieces = []
            for unit in range(depth // SPAN):
                taken = ref[kind, pl.ds(base + unit, group)]
                pieces.append(taken.reshape(group * rows, SPAN))
            return jnp.concatenate(pieces, axis=1)

        products = []
        for kind in range(3):
            upper, lower = gathered(high, kind), gathered(low, kind)
            near = table[:, kind * SPAN : (kind + 1) * SPAN]
            far = table[:, (3 + kind) * SPAN : (4 + kind) * SPAN]
            both = jnp.dot(upper, near, preferred_element_type=F32)
            both += jnp.dot(lower, near, preferred_element_type=F32)
            both += jnp.dot(upper, far, preferred_element_type=F32)
            products.append(both)
        real = (products[0] - products[2]).reshape(group, 2, bins, SPAN)
        imag = (products[0] - products[1]).reshape(group, 2, bins, SPAN)
        for k in range(group):
            at = pl.ds(pl.multiple_of((base + k) * SPAN + HALF, HALF), SPAN)
            for side in range(2):
                image[2 * side, :, at] = real[k, side]
                image[2 * side + 1, :, at] = imag[k, side]

    block = math.gcd(lines_all, 1024)
    length = block + 2 * HALF
    shift = jnp.where(offs_ref[0] < 0, offs_ref[0] + length, offs_ref[0])

    @pl.loop(0, lines_all // block)
    def _(step):
        start = pl.multiple_of(step * block, HALF)
        at = pl.ds(start, length)
        for row in range(0, bins, 8):
            here = slice(row, row + 8)
            a, b = image[0, here, at], image[1, here, at]
            c = pltpu.roll(image[2, here, at], shift, 1)
            d = pltpu.roll(image[3, here, at], shift, 1)
            fields = (a * c + b * d, b * c - a * d, a * a + b * b, c * c + d * d)
            for k, value in enumerate(fields):
                line = lax.broadcasted_iota(jnp.int32, (8, length), 1) + (start - HALF)
                if k == 3:
                    value = jnp.where((line >= 0) & (line < lines_all), value, 0.0)
                for hop in (1, 2, length - 4):
                    value = value + pltpu.roll(value, hop, 1)
                out[k, here, pl.ds(start, block)] = value[:, HALF : HALF + block]


def azimuth_focus(depth, offsets, got, table):
    sources, _, bins, width = got.shape
    windows = sources * width // SPAN
    lines_all = windows * SPAN
    group = math.gcd(windows, 32)
    smem, vmem = pl.BlockSpec(memory_space=pltpu.SMEM), pl.BlockSpec(memory_space=pltpu.VMEM)
    block = pl.BlockSpec((sources, 4, 8, width), lambda i: (0, 0, i, 0))
    store = pltpu.VMEM((3, windows + depth // SPAN - 1, 16, SPAN), BF16)
    flops = 2 * 3 * 3 * windows * 2 * bins * depth * SPAN
    return pl.pallas_call(
        functools.partial(azimuth_kernel, depth, group),
        out_shape=jax.ShapeDtypeStruct((4, bins, lines_all), F32),
        grid=(bins // 8,),
        in_specs=[smem, block, vmem],
        out_specs=pl.BlockSpec((4, 8, lines_all), lambda i: (0, i, 0)),
        scratch_shapes=[
            store,
            store,
            pltpu.VMEM((4, 8, lines_all + 2 * HALF), F32),
        ],
        compiler_params=pltpu.CompilerParams(vmem_limit_bytes=ROOMY),
        cost_estimate=pl.CostEstimate(flops=flops, bytes_accessed=8 << 20, transcendentals=0),
        name="azimuths",
    )(offsets, got, table)


def finish_kernel(bins, start, eights, below_ref, above_ref, *refs):
    *parts, picture, coherence, held = refs
    size = coherence.shape[0]
    held[:, 4:8] = below_ref[...]
    held[:, 8 + bins : 12 + bins] = above_ref[...]
    for eight, part in zip(eights, parts):
        held[:, 8 + eight : 16 + eight] = part[...]
    sums = []
    for field in range(4):
        total = held[field, start : start + size + 16]
        for hop in (1, 2, size + 12):
            total = total + pltpu.roll(total, hop, 0)
        sums.append(total[8 : 8 + size])
    picture[0] = sums[0] * (1.0 / 64.0)
    picture[1] = sums[1] * (1.0 / 64.0)
    strength = jnp.sqrt(sums[0] * sums[0] + sums[1] * sums[1])
    coherence[...] = strength / jnp.sqrt(sums[2] * sums[3] + 1.0)


def finish(bins, start, size, parts, routes, borders, before=()):
    lines_all = parts[0].shape[2]
    block = math.gcd(lines_all, 2048)
    every = range(max(0, (start - 3) // 8), min(bins // 8, (start + size + 3) // 8 + 1))
    eights = [8 * k for k in every]
    operands, specs = list(borders), [pl.BlockSpec((4, 4, block), lambda i: (0, 0, i))] * 2
    for eight in eights:
        chunk, slot = routes[eight]
        operands.append(parts[chunk])
        specs.append(pl.BlockSpec((4, 8, block), lambda i, slot=slot: (0, slot, i)))
    index = start // size
    given = len(operands)

    def kernel(*refs):
        finish_kernel(bins, start, eights, *refs[:given], *refs[given + len(before) :])

    return pl.pallas_call(
        kernel,
        grid=(lines_all // block,),
        out_shape=[
            jax.ShapeDtypeStruct((2, bins, lines_all), F32),
            jax.ShapeDtypeStruct((bins, lines_all), F32),
        ],
        in_specs=specs + [pl.BlockSpec(memory_space=pl.ANY)] * len(before),
        out_specs=[
            pl.BlockSpec((2, size, block), lambda i: (0, index, i)),
            pl.BlockSpec((size, block), lambda i: (index, i)),
        ],
        scratch_shapes=[pltpu.VMEM((4, bins + 16, block), F32)],
        input_output_aliases={given: 0, given + 1: 1} if before else {},
        compiler_params=pltpu.CompilerParams(vmem_limit_bytes=ROOMY),
        cost_estimate=pl.CostEstimate(
            flops=3000 * size * lines_all, bytes_accessed=16 << 20, transcendentals=0
        ),
        name="finish",
    )(*operands, *before)


def arrangement(bins):
    if bins < 64:
        every = tuple(range(0, bins, 8))
        return [every], [[(0, every)]]
    chunks = [(0, bins - 8), (8, 16, 24, 32), (40, 48)]
    return chunks, [[(0, (0, bins - 8))], [(8, (8, 16)), (8, (24, 32))], [(8, (40, 48))]]


def on_device(raw_first, raw_second, offsets, chirp_lengths):
    count = lax.axis_size("az")
    lines, range_count = raw_first.shape[1:]
    lines_all = lines * count
    reach = min(range_count, lines_all) // 4
    bins = WINDOW // count
    share = SPAN // bins
    plan = ((0, reach + SPAN), (HALF, reach + 2 * SPAN))
    chunks, calls = arrangement(bins)
    routes = {eight: (k, slot) for k, chunk in enumerate(chunks) for slot, eight in enumerate(chunk)}

    def columns(starts):
        return tuple(bins * k + start for k in range(share) for start in starts)

    def pair(starts, spare):
        return tuple(
            (0, side, lead + spare, depth + spare, columns(starts))
            for side, (lead, depth) in enumerate(plan)
        )

    def turned(got):
        width = got.shape[3]
        if width % SPAN:
            fold = SPAN // width
            got = got.reshape(count // fold, fold, 4, got.shape[2], width)
            got = got.transpose(0, 2, 3, 1, 4).reshape(count // fold, 4, got.shape[3], SPAN)
        return got

    along = ((1, 0, 0, plan[0][1], tuple(8 * k for k in range(SPAN // 8))),)
    head = make_tables(pair(chunks[0], 0), offsets, chirp_lengths)
    sent, given, ready = {}, offsets, head
    exchanged = []
    for index, call in enumerate(calls):
        if index == 1:
            ready = make_tables(pair(call[0][1], HALF), given, chirp_lengths)
        spare = HALF if index else 0
        groups = [(spare - (eights[0] - start) if index else 0, eights) for start, eights in call]
        local = {}
        owners = sorted({routes[eight][0] for _, eights in call for eight in eights})
        for _, eights in call:
            for eight in eights:
                chunk, slot = routes[eight]
                local[eight] = (owners.index(chunk), slot)
        results = range_focus(
            plan, share, groups, local, index > 1, count, given, raw_first, raw_second, ready
        )
        for owner, result in zip(owners, results):
            sent[owner] = result
        given, sent[owners[0]] = lax.optimization_barrier((given, sent[owners[0]]))
        if index < 2:
            exchanged.append(exchange(sent[index], exchanged))
        if index == 0:
            continue
        if index == 1:
            given = lax.optimization_barrier((given, exchanged[0]))[0]
    base = make_tables(along, given, chirp_lengths)[0]
    up = [(i, i + 1) for i in range(count - 1)]
    down = [(j, i) for i, j in up]
    parts, borders = [], None
    for index in range(len(chunks)):
        if index >= len(exchanged):
            earlier = (parts[index - 2], borders) if index > 1 else (given, borders)
            sent[index], earlier = lax.optimization_barrier((sent[index], earlier))
            if index > 1:
                parts[index - 2], borders = earlier
            exchanged.append(exchange(sent[index], exchanged))
        if index:
            parts.append(azimuth_focus(plan[0][1], offsets, turned(exchanged[index - 1]), base))
        if index == 1:
            borders = bordering(parts[0], up, down)
    parts.append(azimuth_focus(plan[0][1], offsets, turned(exchanged[-1]), base))
    if len(chunks) == 1:
        borders = bordering(parts[0], up, down)
        return tuple(finish(bins, 0, bins, parts, routes, borders))
    outs = finish(bins, 0, bins // 2, parts, routes, borders)
    return tuple(finish(bins, bins // 2, bins // 2, parts, routes, borders, tuple(outs)))


def bordering(part, up, down):
    below = lax.ppermute(part[:, part.shape[1] - 4 :], "az", up)
    return below, lax.ppermute(part[:, 0:4], "az", down)


def exchange(value, earlier):
    if earlier:
        value, earlier[-1] = lax.optimization_barrier((value, earlier[-1]))
    return lax.all_to_all(value, "az", split_axis=0, concat_axis=0, tiled=True)


def solution(mesh):
    in_specs = (P("groups", "az", None), P("groups", "az", None), P("groups"), P("groups"))
    out_specs = (P("groups", "az", None), P(("groups", "az"), None))
    return jax.shard_map(
        on_device, mesh=mesh, in_specs=in_specs, out_specs=out_specs, check_vma=False
    )
```

```python
import functools
import math

import jax
import jax.numpy as jnp
from jax import lax
from jax.experimental import pallas as pl
from jax.experimental.pallas import tpu as pltpu
from jax.sharding import PartitionSpec as P

WINDOW = 1024
MAXSHIFT = 16
SPAN = 256
HALF = 128
LIMIT = 60 * 1024 * 1024
ROOMY = 22 * 1024 * 1024

F32, BF16 = jnp.float32, jnp.bfloat16


def chirp_lines(length, depth):
    shape = (8, depth)
    sample = lax.broadcasted_iota(jnp.int32, shape, 1) - lax.broadcasted_iota(jnp.int32, shape, 0)
    held = (sample >= 0) & (sample < length)
    offset = jnp.where(held, 2 * sample - length, 0)
    square = offset * offset
    period = jnp.full(shape, 8 * length, jnp.int32)
    whole = (square.astype(F32) / period.astype(F32)).astype(jnp.int32)
    numerator = square - whole * period
    numerator = jnp.where(numerator < 0, numerator + period, numerator)
    numerator = jnp.where(numerator >= period, numerator - period, numerator)
    size = period.astype(F32) * 0.125
    angles = jnp.pi * numerator.astype(F32) / (4.0 * size)
    amplitude = jnp.where(held, 1.0 / jnp.sqrt(size), 0.0)
    return amplitude * jnp.cos(angles), amplitude * jnp.sin(angles)


def table_kernel(plan, offs_ref, lengths_ref, *refs):
    outs, scratch = refs[:-1], refs[-1]
    deepest = max(item[3] for item in plan)
    lines = {row: chirp_lines(lengths_ref[row], deepest) for row in {item[0] for item in plan}}
    for (row, shifted, lead, depth, starts), out in zip(plan, outs):
        cols = 8 * len(starts)
        base = lead - offs_ref[1] if shifted else lead
        uniform = len(starts) > 8 and all(start == 8 * k for k, start in enumerate(starts))
        for part, line in enumerate(lines[row]):
            line = line[:, 0:depth]
            if uniform:
                held = line

                @pl.loop(0, len(starts))
                def _(k):
                    moved = pltpu.roll(held, base + 8 * k, 1)
                    scratch[pl.ds(pl.multiple_of(part * cols + 8 * k, 8), 8), 0:depth] = moved

            else:
                for k, start in enumerate(starts):
                    moved = pltpu.roll(line, base + start, 1)
                    scratch[part * cols + 8 * k : part * cols + 8 * k + 8, 0:depth] = moved

        @pl.loop(0, depth // HALF, unroll=2)
        def _(k):
            at = pl.ds(pl.multiple_of(k * HALF, HALF), HALF)
            turned = scratch[0 : 2 * cols, at].T
            if row:
                real, imag = turned[:, 0:cols], turned[:, cols:]
                turned = jnp.concatenate([real, real + imag, real - imag], axis=1)
            width = turned.shape[1]
            high = turned.astype(BF16)
            out[at, 0:width] = high
            out[at, width : 2 * width] = (turned - high.astype(F32)).astype(BF16)


def make_tables(plan, offsets, lengths):
    rows = max(2 * 8 * len(item[4]) for item in plan)
    depth = max(item[3] for item in plan)
    widths = [8 * len(item[4]) * (6 if item[0] else 4) for item in plan]
    size = sum(item[3] * width for item, width in zip(plan, widths))
    smem = pl.BlockSpec(memory_space=pltpu.SMEM)
    vmem = pl.BlockSpec(memory_space=pltpu.VMEM)
    return pl.pallas_call(
        functools.partial(table_kernel, plan),
        out_shape=[jax.ShapeDtypeStruct((item[3], width), BF16) for item, width in zip(plan, widths)],
        in_specs=[smem, smem],
        out_specs=[vmem] * len(plan),
        scratch_shapes=[pltpu.VMEM((rows, depth), F32)],
        compiler_params=pltpu.CompilerParams(vmem_limit_bytes=ROOMY if plan[0][0] else LIMIT),
        cost_estimate=pl.CostEstimate(flops=size * 400, bytes_accessed=2 * size, transcendentals=0),
        name="tables",
    )(offsets, lengths)


def range_kernel(plan, windows, share, groups, routes, looped, offs_ref, first_ref, second_ref, *refs):
    tables, outs = refs[0:2], refs[2:]
    lines = first_ref.shape[1]
    for side, (source, table) in enumerate(zip((first_ref, second_ref), tables)):
        lead, depth = plan[side]

        def run(window, source=source, table=table, side=side, lead=lead, depth=depth):
            still = isinstance(window, int)
            start = SPAN * window - lead
            if still and start < 0:
                empty = jnp.zeros((2 * lines, -start), BF16)
                inner = source[:, :, 0 : start + depth].reshape(2 * lines, start + depth)
                left = jnp.concatenate([empty, inner], axis=1)
            else:
                at = pl.ds(start if still else pl.multiple_of(start, HALF), depth)
                left = source[:, :, at].reshape(2 * lines, depth)
            for skip, eights in groups:
                cols = share * len(eights) * 8
                both = jnp.dot(left, table[skip : skip + depth], preferred_element_type=F32)
                turned = (both[:, 0 : 2 * cols] + both[:, 2 * cols :]).T
                real = turned[0:cols, 0:lines] + turned[cols:, lines:]
                imag = turned[0:cols, lines:] - turned[cols:, 0:lines]
                real = real.reshape(share, len(eights), 8, lines)
                imag = imag.reshape(share, len(eights), 8, lines)
                for k, eight in enumerate(eights):
                    pair = real[:, k], imag[:, k]
                    if side and still and window * SPAN + eight < MAXSHIFT:
                        shape = (share, 8, lines)
                        index = lax.broadcasted_iota(jnp.int32, shape, 0) * (SPAN // share)
                        index = index + lax.broadcasted_iota(jnp.int32, shape, 1)
                        inside = index + (window * SPAN + eight) >= offs_ref[1]
                        pair = [jnp.where(inside, value, 0.0) for value in pair]
                    chunk, slot = routes[eight]
                    for part, value in enumerate(pair):
                        place = pl.ds(window * share, share)
                        outs[chunk][place, 2 * side + part, 8 * slot : 8 * slot + 8] = value

        if looped:
            for window in range(side):
                run(window)
            pl.loop(side, windows)(run)
        else:
            for window in range(windows):
                run(window)


def range_focus(plan, share, groups, routes, looped, count, offsets, first, second, tables):
    windows = WINDOW // SPAN
    lines_all = first.shape[1]
    lines = min(lines_all, SPAN)
    reach = max(SPAN * (windows - 1) - lead + depth for lead, depth in plan)
    block = pl.BlockSpec((2, lines, reach), lambda i: (0, i, 0))
    whole = pl.BlockSpec(memory_space=pltpu.VMEM)
    sizes = [0] * (1 + max(chunk for chunk, _ in routes.values()))
    for chunk, _ in routes.values():
        sizes[chunk] += 8
    bins = sum(sizes)
    flops = sum(2 * 2 * lines_all * windows * depth * share * bins * 4 for _, depth in plan)
    return pl.pallas_call(
        functools.partial(range_kernel, plan, windows, share, groups, routes, looped),
        grid=(lines_all // lines,),
        out_shape=[jax.ShapeDtypeStruct((count, 4, size, lines_all), F32) for size in sizes],
        in_specs=[pl.BlockSpec(memory_space=pltpu.SMEM), block, block, whole, whole],
        out_specs=[pl.BlockSpec((count, 4, size, lines), lambda i: (0, 0, 0, i)) for size in sizes],
        compiler_params=pltpu.CompilerParams(vmem_limit_bytes=LIMIT),
        cost_estimate=pl.CostEstimate(flops=flops, bytes_accessed=16 << 20, transcendentals=0),
        name="ranges",
    )(offsets, first, second, *tables)


def azimuth_kernel(depth, group, offs_ref, got_ref, table, out, high, low, image):
    sources, _, bins, width = got_ref.shape
    spans = width // SPAN
    windows = sources * spans
    lines_all = windows * SPAN
    extra = high.shape[1] - windows
    rows = 2 * bins

    @pl.loop(0, sources)
    def _(source):
        for part in range(spans):
            at = slice(part * SPAN, (part + 1) * SPAN)
            real = jnp.concatenate([got_ref[source, 0, :, at], got_ref[source, 2, :, at]], axis=0)
            imag = jnp.concatenate([got_ref[source, 1, :, at], got_ref[source, 3, :, at]], axis=0)
            for kind, value in enumerate((real + imag, real, imag)):
                upper = value.astype(BF16)
                high[kind, source * spans + part] = upper
                low[kind, source * spans + part] = (value - upper.astype(F32)).astype(BF16)

    for kind in range(3):
        for slot in range(extra):
            high[kind, windows + slot] = high[kind, slot % windows]
            low[kind, windows + slot] = low[kind, slot % windows]

    pads = jnp.zeros((4, bins, HALF), F32)
    image[:, :, 0:HALF] = pads
    image[:, :, HALF + lines_all :] = pads

    @pl.loop(0, windows // group)
    def _(turn):
        base = turn * group

        def gathered(ref, kind):
            pieces = []
            for unit in range(depth // SPAN):
                taken = ref[kind, pl.ds(base + unit, group)]
                pieces.append(taken.reshape(group * rows, SPAN))
            return jnp.concatenate(pieces, axis=1)

        products = []
        for kind in range(3):
            upper, lower = gathered(high, kind), gathered(low, kind)
            near = table[:, kind * SPAN : (kind + 1) * SPAN]
            far = table[:, (3 + kind) * SPAN : (4 + kind) * SPAN]
            both = jnp.dot(upper, near, preferred_element_type=F32)
            both += jnp.dot(lower, near, preferred_element_type=F32)
            both += jnp.dot(upper, far, preferred_element_type=F32)
            products.append(both)
        real = (products[0] - products[2]).reshape(group, 2, bins, SPAN)
        imag = (products[0] - products[1]).reshape(group, 2, bins, SPAN)
        for k in range(group):
            at = pl.ds(pl.multiple_of((base + k) * SPAN + HALF, HALF), SPAN)
            for side in range(2):
                image[2 * side, :, at] = real[k, side]
                image[2 * side + 1, :, at] = imag[k, side]

    block = math.gcd(lines_all, 1024)
    length = block + 2 * HALF
    shift = jnp.where(offs_ref[0] < 0, offs_ref[0] + length, offs_ref[0])

    @pl.loop(0, lines_all // block)
    def _(step):
        start = pl.multiple_of(step * block, HALF)
        at = pl.ds(start, length)
        for row in range(0, bins, 8):
            here = slice(row, row + 8)
            a, b = image[0, here, at], image[1, here, at]
            c = pltpu.roll(image[2, here, at], shift, 1)
            d = pltpu.roll(image[3, here, at], shift, 1)
            fields = (a * c + b * d, b * c - a * d, a * a + b * b, c * c + d * d)
            for k, value in enumerate(fields):
                line = lax.broadcasted_iota(jnp.int32, (8, length), 1) + (start - HALF)
                if k == 3:
                    value = jnp.where((line >= 0) & (line < lines_all), value, 0.0)
                for hop in (1, 2, length - 4):
                    value = value + pltpu.roll(value, hop, 1)
                out[k, here, pl.ds(start, block)] = value[:, HALF : HALF + block]


def azimuth_focus(depth, offsets, got, table):
    sources, _, bins, width = got.shape
    windows = sources * width // SPAN
    lines_all = windows * SPAN
    group = math.gcd(windows, 32)
    smem, vmem = pl.BlockSpec(memory_space=pltpu.SMEM), pl.BlockSpec(memory_space=pltpu.VMEM)
    block = pl.BlockSpec((sources, 4, 8, width), lambda i: (0, 0, i, 0))
    store = pltpu.VMEM((3, windows + depth // SPAN - 1, 16, SPAN), BF16)
    flops = 2 * 3 * 3 * windows * 2 * bins * depth * SPAN
    return pl.pallas_call(
        functools.partial(azimuth_kernel, depth, group),
        out_shape=jax.ShapeDtypeStruct((4, bins, lines_all), F32),
        grid=(bins // 8,),
        in_specs=[smem, block, vmem],
        out_specs=pl.BlockSpec((4, 8, lines_all), lambda i: (0, i, 0)),
        scratch_shapes=[
            store,
            store,
            pltpu.VMEM((4, 8, lines_all + 2 * HALF), F32),
        ],
        compiler_params=pltpu.CompilerParams(vmem_limit_bytes=ROOMY),
        cost_estimate=pl.CostEstimate(flops=flops, bytes_accessed=8 << 20, transcendentals=0),
        name="azimuths",
    )(offsets, got, table)


def finish_kernel(bins, start, eights, below_ref, above_ref, *refs):
    *parts, picture, coherence, held = refs
    size = coherence.shape[0]
    held[:, 4:8] = below_ref[...]
    held[:, 8 + bins : 12 + bins] = above_ref[...]
    for eight, part in zip(eights, parts):
        held[:, 8 + eight : 16 + eight] = part[...]
    sums = []
    for field in range(4):
        total = held[field, start : start + size + 16]
        for hop in (1, 2, size + 12):
            total = total + pltpu.roll(total, hop, 0)
        sums.append(total[8 : 8 + size])
    picture[0] = sums[0] * (1.0 / 64.0)
    picture[1] = sums[1] * (1.0 / 64.0)
    strength = jnp.sqrt(sums[0] * sums[0] + sums[1] * sums[1])
    coherence[...] = strength / jnp.sqrt(sums[2] * sums[3] + 1.0)


def finish(bins, start, size, parts, routes, borders, before=()):
    lines_all = parts[0].shape[2]
    block = math.gcd(lines_all, 2048)
    every = range(max(0, (start - 3) // 8), min(bins // 8, (start + size + 3) // 8 + 1))
    eights = [8 * k for k in every]
    operands, specs = list(borders), [pl.BlockSpec((4, 4, block), lambda i: (0, 0, i))] * 2
    for eight in eights:
        chunk, slot = routes[eight]
        operands.append(parts[chunk])
        specs.append(pl.BlockSpec((4, 8, block), lambda i, slot=slot: (0, slot, i)))
    index = start // size
    given = len(operands)

    def kernel(*refs):
        finish_kernel(bins, start, eights, *refs[:given], *refs[given + len(before) :])

    return pl.pallas_call(
        kernel,
        grid=(lines_all // block,),
        out_shape=[
            jax.ShapeDtypeStruct((2, bins, lines_all), F32),
            jax.ShapeDtypeStruct((bins, lines_all), F32),
        ],
        in_specs=specs + [pl.BlockSpec(memory_space=pl.ANY)] * len(before),
        out_specs=[
            pl.BlockSpec((2, size, block), lambda i: (0, index, i)),
            pl.BlockSpec((size, block), lambda i: (index, i)),
        ],
        scratch_shapes=[pltpu.VMEM((4, bins + 16, block), F32)],
        input_output_aliases={given: 0, given + 1: 1} if before else {},
        compiler_params=pltpu.CompilerParams(vmem_limit_bytes=ROOMY),
        cost_estimate=pl.CostEstimate(
            flops=3000 * size * lines_all, bytes_accessed=16 << 20, transcendentals=0
        ),
        name="finish",
    )(*operands, *before)


def arrangement(bins):
    if bins < 64:
        every = tuple(range(0, bins, 8))
        return [every], [[(0, every)]]
    chunks = [(0, bins - 8), (8, 16, 24, 32), (40, 48)]
    return chunks, [[(0, (0, bins - 8))], [(8, (8, 16)), (8, (24, 32))], [(8, (40, 48))]]


def on_device(raw_first, raw_second, offsets, chirp_lengths):
    count = lax.axis_size("az")
    lines, range_count = raw_first.shape[1:]
    lines_all = lines * count
    reach = min(range_count, lines_all) // 4
    bins = WINDOW // count
    share = SPAN // bins
    plan = ((0, reach + SPAN), (HALF, reach + 2 * SPAN))
    chunks, calls = arrangement(bins)
    routes = {eight: (k, slot) for k, chunk in enumerate(chunks) for slot, eight in enumerate(chunk)}

    def columns(starts):
        return tuple(bins * k + start for k in range(share) for start in starts)

    def pair(starts, spare):
        return tuple(
            (0, side, lead + spare, depth + spare, columns(starts))
            for side, (lead, depth) in enumerate(plan)
        )

    def turned(got):
        width = got.shape[3]
        if width % SPAN:
            fold = SPAN // width
            got = got.reshape(count // fold, fold, 4, got.shape[2], width)
            got = got.transpose(0, 2, 3, 1, 4).reshape(count // fold, 4, got.shape[3], SPAN)
        return got

    along = ((1, 0, 0, plan[0][1], tuple(8 * k for k in range(SPAN // 8))),)
    head = make_tables(pair(chunks[0], 0), offsets, chirp_lengths)
    sent, given, ready = {}, offsets, head
    exchanged = []
    for index, call in enumerate(calls):
        if index == 1:
            ready = make_tables(pair(call[0][1], HALF), given, chirp_lengths)
        spare = HALF if index else 0
        groups = [(spare - (eights[0] - start) if index else 0, eights) for start, eights in call]
        local = {}
        owners = sorted({routes[eight][0] for _, eights in call for eight in eights})
        for _, eights in call:
            for eight in eights:
                chunk, slot = routes[eight]
                local[eight] = (owners.index(chunk), slot)
        results = range_focus(
            plan, share, groups, local, index > 1, count, given, raw_first, raw_second, ready
        )
        for owner, result in zip(owners, results):
            sent[owner] = result
        given, sent[owners[0]] = lax.optimization_barrier((given, sent[owners[0]]))
        if index < 2:
            exchanged.append(exchange(sent[index], exchanged))
        if index == 0:
            continue
        if index == 1:
            given = lax.optimization_barrier((given, exchanged[0]))[0]
    base = make_tables(along, given, chirp_lengths)[0]
    up = [(i, i + 1) for i in range(count - 1)]
    down = [(j, i) for i, j in up]
    parts, borders = [], None
    for index in range(len(chunks)):
        if index >= len(exchanged):
            earlier = (parts[index - 2], borders) if index > 1 else (given, borders)
            sent[index], earlier = lax.optimization_barrier((sent[index], earlier))
            if index > 1:
                parts[index - 2], borders = earlier
            exchanged.append(exchange(sent[index], exchanged))
        if index:
            parts.append(azimuth_focus(plan[0][1], offsets, turned(exchanged[index - 1]), base))
        if index == 1:
            borders = bordering(parts[0], up, down)
    parts.append(azimuth_focus(plan[0][1], offsets, turned(exchanged[-1]), base))
    if len(chunks) == 1:
        borders = bordering(parts[0], up, down)
        return tuple(finish(bins, 0, bins, parts, routes, borders))
    outs = finish(bins, 0, bins // 2, parts, routes, borders)
    return tuple(finish(bins, bins // 2, bins // 2, parts, routes, borders, tuple(outs)))


def bordering(part, up, down):
    below = lax.ppermute(part[:, part.shape[1] - 4 :], "az", up)
    return below, lax.ppermute(part[:, 0:4], "az", down)


def exchange(value, earlier):
    if earlier:
        value, earlier[-1] = lax.optimization_barrier((value, earlier[-1]))
    return lax.all_to_all(value, "az", split_axis=0, concat_axis=0, tiled=True)


def solution(mesh):
    in_specs = (P("groups", "az", None), P("groups", "az", None), P("groups"), P("groups"))
    out_specs = (P("groups", "az", None), P(("groups", "az"), None))
    return jax.shard_map(
        on_device, mesh=mesh, in_specs=in_specs, out_specs=out_specs, check_vma=False
    )
```
